32 devices in a mesh: dp: 8 (over y, x, core), tensor: 4 (over z).
Axes of the slice: x: 2, y: 2, z: 4, core: 2. Of those that a mesh axis runs over, the one named last changes fastest.
Arguments:
- inputs: bfloat16 [4, 4096, 768], P(None, ('dp', 'tensor')), may hold values from -12 to 12
- cotangent: bfloat16 [4, 4096, 768], P(None, ('dp', 'tensor')), may hold values from -12 to 12
- segment_ids: int32 [4, 8, 512], P(None, 'dp'), may hold values from 0 to 23, never falling along the last dimension, each value on 1 to 48 neighbouring positions
- ln1_gain: float32 [768], replicated, may hold values from 0.25 to 1.75
- ln1_bias: float32 [768], replicated, may hold values from -1.75 to 1.75
- qkv_weight: bfloat16 [3, 768, 768], P(None, 'dp', 'tensor'), may hold values from -0.21875 to 0.21875
- qv_bias: float32 [2, 768], P(None, 'tensor'), may hold values from -1.75 to 1.75
- out_weight: bfloat16 [768, 768], P('tensor', 'dp'), may hold values from -0.4375 to 0.4375
- out_bias: float32 [768], replicated, may hold values from -1.75 to 1.75
- ln2_gain: float32 [768], replicated, may hold values from 0.25 to 1.75
- ln2_bias: float32 [768], replicated, may hold values from -1.75 to 1.75
- up_weight: bfloat16 [768, 3072], P('dp', 'tensor'), may hold values from -0.21875 to 0.21875
- up_bias: float32 [3072], P('tensor'), may hold values from -1.75 to 1.75
- down_weight: bfloat16 [3072, 768], P('tensor', 'dp'), may hold values from -0.109375 to 0.109375
- down_bias: float32 [768], replicated, may hold values from -1.75 to 1.75
Outputs:
- outputs: float32 [4, 4096, 768], P(None, ('dp', 'tensor'))
- input_grad: float32 [4, 4096, 768], P(None, ('dp', 'tensor'))
- ln1_gain_grad: float32 [768], replicated
- ln1_bias_grad: float32 [768], replicated
- qkv_weight_grad: float32 [3, 768, 768], P(None, 'dp', 'tensor')
- qv_bias_grad: float32 [2, 768], replicated
- out_weight_grad: float32 [768, 768], P('tensor', 'dp')
- out_bias_grad: float32 [768], replicated
- ln2_gain_grad: float32 [768], replicated
- ln2_bias_grad: float32 [768], replicated
- up_weight_grad: float32 [768, 3072], P('dp', 'tensor')
- up_bias_grad: float32 [3072], replicated
- down_weight_grad: float32 [3072, 768], P('tensor', 'dp')
- down_bias_grad: float32 [768], replicated
The draws below stay inside these ranges and needn't reach their ends.
Inputs may be any that keep to these rules, and one draw needn't show every extreme that they name: `segment_ids`: along each sequence of 512 tokens the ids never fall; a caption spans 1 to 48 tokens, and one caption of each sequence exactly 48.
All inputs are finite; a program needn't handle non-finite values.
Results may differ from the reference program's by a relative error of at most 0.017.
Values may be sent and summed in bfloat16 or wider, within the bound.
A program may use at most 192 MiB of HBM per device.

```python
import math
import jax
import jax.numpy as jnp
import numpy as np
from jax import lax

D = 768
H = 12
HD = 64
FF = 3072
LEN = 512
MICRO = 4
SEQ_MB = 1
SEGS = 24
MOST = 48
NSEQ = 8
TOK_MB = 4096
N_DP = 8


def strengthened(values, own_key, source, target, blocks, factor):
    owner, partner = [(jnp.arange(values.shape[dim]) // (values.shape[dim] // blocks)).reshape([-1 if axis == dim else 1 for axis in range(values.ndim)]) for dim in (source, target)]
    chosen = jax.random.permutation(own_key, blocks)[partner]
    strong = (owner == chosen) | (owner == (partner + blocks // 2) % blocks)
    return jnp.where(strong, factor * values, values)


def block_scale(own_key, dims, shards, low, largest):
    def one(position, parts):
        draws = jax.random.uniform(jax.random.fold_in(jax.random.fold_in(own_key, 6), position), (parts,), jnp.float32, low / len(shards), largest / len(shards))
        return jnp.repeat(jnp.exp(draws), dims[position] // parts).reshape((-1,) + (1,) * (len(dims) - position - 1))

    gain = one(*shards[0])
    for cut in shards[1:]:
        gain = gain * one(*cut)
    return gain


def profile(amount, total, limit, lean):
    weights = [(1 << 20) // math.isqrt(rank ** lean) + 1 for rank in range(2, amount + 1)]
    rest, holding = total - limit - (amount - 1), [1] * (amount - 1)
    while rest > 0:
        candidates = [i for i in range(amount - 1) if holding[i] < limit]
        pool, remaining = sum([weights[i] for i in candidates]), rest
        for i in candidates:
            extra = min(limit - holding[i], max(1, remaining * weights[i] // pool), rest)
            holding[i] = holding[i] + extra
            rest = rest - extra
    return np.array([limit] + holding)


def uneven(key, count, total, reach, slope):
    if count == 2:
        one = jax.random.randint(key, (), max(1, total - reach), min(reach, total - 1) + 1)
        return jnp.stack([one, total - one])
    tallies = jnp.asarray(profile(count, total, reach, slope), jnp.int32)
    pairs = (count - 1) // 2
    giver, sink = tallies[1:1 + 2 * pairs:2], tallies[2:2 + 2 * pairs:2]
    room = jnp.minimum(giver - 1, reach - sink)
    passed = jax.random.randint(jax.random.fold_in(key, 1), (pairs,), 0, 1 << 20) % (room + 1)
    tallies = tallies.at[1:1 + 2 * pairs:2].set(giver - passed).at[2:2 + 2 * pairs:2].set(sink + passed)
    return tallies[jax.random.permutation(jax.random.fold_in(key, 2), count)]


def gaussian(own_key, extent, scale, reach, shards=(), dtype=jnp.bfloat16):
    drawn = jax.random.normal(own_key, extent, jnp.float32) * scale
    if len(shards) > 0:
        drawn = block_scale(own_key, extent, shards, -0.22, 0.18) * drawn
    return jnp.clip(drawn, min=-reach, max=reach).astype(dtype)


def gaussian_with(key, extent, width, reach, shards, heavy, kind=jnp.bfloat16):
    values = width * jax.random.normal(key, extent, jnp.float32)
    if shards:
        values = values * block_scale(key, extent, shards, -0.22, 0.18)
    return jnp.clip(strengthened(values, jax.random.fold_in(key, 3), *heavy), -reach, reach).astype(kind)


def setup_inputs(seed: int = 0) -> dict:
    streams_of = jax.random.split(jax.random.key(seed), 16)
    inputs = gaussian_with(streams_of[0], (MICRO, TOK_MB, D), 1.0, 12.0, ((1, 32),), (1, 2, 32, 2.75))
    cotangent = gaussian_with(streams_of[1], (MICRO, TOK_MB, D), 1.0, 12.0, ((1, 32),), (1, 2, 32, 2.75))
    segment_ids = jax.vmap(lambda own: jnp.searchsorted(jnp.cumsum(uneven(own, SEGS, LEN, MOST, 1)), jnp.arange(LEN), side="right"))(jax.random.split(streams_of[2], MICRO * NSEQ)).reshape((MICRO, NSEQ, LEN)).astype(jnp.int32)
    ln1_gain = jnp.clip(1.0 + 0.15 * jax.random.normal(streams_of[3], (D,), jnp.float32), 0.25, 1.75)
    ln1_bias = gaussian(streams_of[4], (D,), 0.3, 1.75, (), jnp.float32)
    qkv_weight = gaussian(streams_of[5], (3, D, D), D ** -0.5, 0.21875, ((1, 8), (2, 4)))
    qv_bias = gaussian(streams_of[6], (2, D), 0.3, 1.75, ((1, 4),), jnp.float32)
    out_weight = gaussian(streams_of[7], (D, D), (D // 4) ** -0.5, 0.4375, ((0, 4), (1, 8)))
    out_bias = gaussian(streams_of[8], (D,), 0.3, 1.75, (), jnp.float32)
    ln2_gain = jnp.clip(1.0 + 0.15 * jax.random.normal(streams_of[9], (D,), jnp.float32), 0.25, 1.75)
    ln2_bias = gaussian(streams_of[10], (D,), 0.3, 1.75, (), jnp.float32)
    up_weight = gaussian(streams_of[11], (D, FF), D ** -0.5, 0.21875, ((0, 8), (1, 4)))
    up_bias = gaussian(streams_of[12], (FF,), 0.3, 1.75, ((0, 4),), jnp.float32)
    down_weight = gaussian(streams_of[13], (FF, D), FF ** -0.5, 0.109375, ((0, 4), (1, 8)))
    down_bias = gaussian(streams_of[14], (D,), 0.3, 1.75, (), jnp.float32)
    return {"inputs": inputs, "cotangent": cotangent, "segment_ids": segment_ids, "ln1_gain": ln1_gain, "ln1_bias": ln1_bias, "qkv_weight": qkv_weight, "qv_bias": qv_bias, "out_weight": out_weight, "out_bias": out_bias, "ln2_gain": ln2_gain, "ln2_bias": ln2_bias, "up_weight": up_weight, "up_bias": up_bias, "down_weight": down_weight, "down_bias": down_bias}


epsilon = 1e-05
masked_value = -1000000000.0
highest = lax.Precision.HIGHEST

@jax.custom_vjp
def low(v):
    return lax.optimization_barrier(v.astype(jnp.bfloat16)).astype(jnp.float32)

@jax.custom_vjp
def low_back(v):
    return v

def low_keep(v):
    return (low(v), None)

def low_pass(kept, grad):
    return (grad,)

def back_keep(v):
    return (v, None)

def back_low(kept, grad):
    return (low(grad),)
low.defvjp(low_keep, low_pass)
low_back.defvjp(back_keep, back_low)

def layer_norm(stream_values, scales, shifts):
    centered = stream_values - lax.optimization_barrier(jnp.mean(stream_values, -1, keepdims=True))
    variance = lax.optimization_barrier(jnp.mean(centered * centered, -1, keepdims=True))
    return centered * lax.rsqrt(variance + epsilon) * scales + shifts

def forward(param_set, stream, segment_ids):
    ln1_gain, ln1_bias, qkv_weight, qv_bias, out_weight, out_bias, ln2_gain, ln2_bias, up_weight, up_bias, down_weight, down_bias = param_set
    groups, length, feature_width = stream.shape
    normed = low(layer_norm(stream, ln1_gain, ln1_bias))

    def project(matrix):
        return jnp.einsum('gld,de->gle', normed, matrix, precision=highest)
    heads_shape = (groups, length, H, HD)
    query = low_back(low(project(qkv_weight[0]) + qv_bias[0])).reshape(heads_shape)
    key_heads = low_back(low(project(qkv_weight[1]))).reshape(heads_shape)
    value_heads = low_back(low(project(qkv_weight[2]) + qv_bias[1])).reshape(heads_shape)
    scores = jnp.einsum('gqhd,gkhd->ghqk', query, key_heads, precision=highest) * HD ** (-0.5)
    same_caption = (segment_ids[:, :, None] == segment_ids[:, None, :])[:, None]
    scores = low_back(jnp.where(same_caption, scores, masked_value))
    shifted = jnp.exp(scores - lax.optimization_barrier(jnp.max(scores, -1, keepdims=True)))
    attention = shifted / lax.optimization_barrier(jnp.sum(shifted, -1, keepdims=True))
    mixed = jnp.einsum('ghqk,gkhd->gqhd', low(attention), value_heads, precision=highest)
    mixed = low_back(low(mixed.reshape(groups, length, feature_width)))
    branch = low_back(jnp.einsum('gld,de->gle', mixed, out_weight, precision=highest) + out_bias)
    middle = stream + branch
    normed_two = low(layer_norm(middle, ln2_gain, ln2_bias))
    hidden = low_back(jnp.einsum('gld,de->gle', normed_two, up_weight, precision=highest) + up_bias)
    active = low(jax.nn.gelu(hidden, approximate=False))
    feed_out = low_back(jnp.einsum('gle,ed->gld', active, down_weight, precision=highest) + down_bias)
    return middle + feed_out

def reference(inputs, cotangent, segment_ids, ln1_gain, ln1_bias, qkv_weight, qv_bias, out_weight, out_bias, ln2_gain, ln2_bias, up_weight, up_bias, down_weight, down_bias):
    param_set = tuple((element.astype(jnp.float32) for element in (ln1_gain, ln1_bias, qkv_weight, qv_bias, out_weight, out_bias, ln2_gain, ln2_bias, up_weight, up_bias, down_weight, down_bias)))
    seq_count = MICRO * SEQ_MB * N_DP
    group_size = math.gcd(seq_count, max(1, 4096 // LEN))
    block_shape = (seq_count // group_size, group_size, LEN, D)
    stacked_in = inputs.astype(jnp.float32).reshape(block_shape)
    stacked_grad = cotangent.astype(jnp.float32).reshape(block_shape)
    stacked_seg = segment_ids.reshape(seq_count // group_size, group_size, LEN)

    def scan_step(running, element):
        block_value, block_grad, block_seg = element
        result, pullback = jax.vjp(lambda params_now, values_now: forward(params_now, values_now, block_seg), param_set, block_value)
        param_grads, value_grads = pullback(block_grad)
        return (jax.tree.map(jnp.add, running, param_grads), (result, value_grads))
    zero_tree = jax.tree.map(jnp.zeros_like, param_set)
    totals, (result, value_grads) = lax.scan(scan_step, zero_tree, (stacked_in, stacked_grad, stacked_seg))
    return (result.reshape(MICRO, TOK_MB, D), value_grads.reshape(MICRO, TOK_MB, D), totals[0], totals[1], totals[2], totals[3], totals[4], totals[5], totals[6], totals[7], totals[8], totals[9], totals[10], totals[11])
```

```python
import functools

import jax
import jax.numpy as jnp
from jax import lax
from jax.experimental import pallas as pl
from jax.experimental.pallas import tpu as pltpu
from jax.sharding import PartitionSpec as P

HD = 64
HALO = 48

epsilon = 1e-05
masked_value = -1000000000.0
bf16, f32 = jnp.bfloat16, jnp.float32


def dot(left, right, left_dim, right_dim):
    return lax.dot_general(
        left, right, (((left_dim,), (right_dim,)), ((), ())), preferred_element_type=f32
    )


def norm_stats(values):
    centered = values - jnp.mean(values, -1, keepdims=True)
    rate = lax.rsqrt(jnp.mean(centered * centered, -1, keepdims=True) + epsilon)
    return centered * rate, rate


def norm_back(grad, hat, rate, gain):
    scaled = grad * gain
    return rate * (
        scaled
        - jnp.mean(scaled, -1, keepdims=True)
        - hat * jnp.mean(scaled * hat, -1, keepdims=True)
    )


def head_base(head, heads_shard, head_cols):
    return (head // heads_shard) * 3 * head_cols + (head % heads_shard) * HD


def probs_of(query, key, same):
    scores = jnp.where(same, dot(query, key, 1, 1) * HD ** (-0.5), masked_value)
    shifted = jnp.exp(scores - jnp.max(scores, -1, keepdims=True))
    return shifted / jnp.sum(shifted, -1, keepdims=True)


def attend_kernel(heads, head_cols, rows, column_ref, row_ref, qkv_ref, mixed_ref):
    same = column_ref[0][HALO : HALO + rows] == row_ref[0]
    for head in range(heads):
        base = head_base(head, head_cols // HD, head_cols)
        query = qkv_ref[0, HALO : HALO + rows, base : base + HD]
        key = qkv_ref[0, :, base + head_cols : base + head_cols + HD]
        value = qkv_ref[0, :, base + 2 * head_cols : base + 2 * head_cols + HD]
        probs_low = probs_of(query, key, same).astype(bf16)
        mixed_ref[0, :, head * HD : (head + 1) * HD] = dot(probs_low, value, 1, 0).astype(bf16)


def attend_back_kernel(heads, head_cols, rows, column_ref, row_ref, qkv_ref, grad_ref, out_ref):
    same = column_ref[0] == row_ref[0]
    own = slice(HALO, HALO + rows)
    for head in range(heads):
        base = head_base(head, head_cols // HD, head_cols)
        query = qkv_ref[0, :, base : base + HD]
        key = qkv_ref[0, :, base + head_cols : base + head_cols + HD]
        value = qkv_ref[0, :, base + 2 * head_cols : base + 2 * head_cols + HD]
        grad = grad_ref[0, :, head * HD : (head + 1) * HD]
        probs = probs_of(query, key, same)
        probs_grad = dot(grad, value, 1, 1)
        scores_grad = probs * (probs_grad - jnp.sum(probs * probs_grad, -1, keepdims=True))
        scores_grad = scores_grad.astype(bf16)
        probs_low = probs.astype(bf16)
        query_grad = dot(scores_grad, key, 1, 0) * HD ** (-0.5)
        key_grad = dot(scores_grad, query, 0, 0) * HD ** (-0.5)
        value_grad = dot(probs_low, grad, 0, 0)
        out_ref[0, :, base : base + HD] = query_grad[own].astype(bf16)
        out_ref[0, :, base + head_cols : base + head_cols + HD] = key_grad[own].astype(bf16)
        out_ref[0, :, base + 2 * head_cols : base + 2 * head_cols + HD] = value_grad[own].astype(bf16)


def one_step(*dims):
    return pl.BlockSpec((1,) + dims, lambda step: (step,) + (0,) * len(dims))


def with_halo(own, first_to_left, last_to_right):
    left = lax.ppermute(own[:, -HALO:], "tensor", last_to_right)
    right = lax.ppermute(own[:, :HALO], "tensor", first_to_left)
    return jnp.concatenate([left, own, right], 1)


def body(
    inputs,
    cotangent,
    segment_ids,
    ln1_gain,
    ln1_bias,
    qkv_weight,
    qv_bias,
    out_weight,
    out_bias,
    ln2_gain,
    ln2_bias,
    up_weight,
    up_bias,
    down_weight,
    down_bias,
):
    batches, rows, width = inputs.shape
    assert segment_ids.shape[1] == 1 and rows >= HALO
    shards = lax.axis_size("tensor")
    replicas = lax.axis_size("dp")
    head_cols = qkv_weight.shape[2]
    hidden_cols = up_weight.shape[1]
    heads = shards * head_cols // HD
    depth = up_weight.shape[0]
    place = lax.axis_index("tensor")
    total = batches * rows
    wide = rows + 2 * HALO

    to_left = [(i, i - 1) for i in range(1, shards)]
    to_right = [(i, i + 1) for i in range(shards - 1)]

    def gather(block):
        whole = lax.all_gather(block, ("tensor", "dp"), axis=0, tiled=True)
        return whole.reshape(shards, width, block.shape[1])

    qkv_all = gather(jnp.transpose(qkv_weight, (1, 0, 2)).reshape(depth, 3 * head_cols))
    out_all = gather(out_weight.T)
    up_all = gather(up_weight)
    down_all = gather(down_weight.T)
    biases = lax.all_gather(
        jnp.concatenate([qv_bias[0], jnp.zeros_like(qv_bias[0]), qv_bias[1], up_bias]), "tensor"
    )
    qkv_bias, up_bias_all = biases[:, : 3 * head_cols], biases[:, 3 * head_cols :]

    ids = jnp.pad(segment_ids[:, 0], ((0, 0), (HALO, HALO)), constant_values=-1)
    ids = lax.dynamic_slice(ids, (0, place * rows), (batches, wide))
    id_column, id_row = ids[:, :, None], ids[:, None, :]

    wide_in = with_halo(inputs, to_left, to_right).astype(f32)
    hat_wide, rate_wide = norm_stats(wide_in)
    normed_wide = (hat_wide * ln1_gain + ln1_bias).astype(bf16)
    normed = normed_wide[:, HALO : HALO + rows].reshape(total, width)
    normed_wide = normed_wide.reshape(batches * wide, width)
    qkv = jnp.concatenate(
        [(dot(normed_wide, qkv_all[t], 1, 0) + qkv_bias[t]).astype(bf16) for t in range(shards)], 1
    ).reshape(batches, wide, 3 * width)
    mixed = pl.pallas_call(
        functools.partial(attend_kernel, heads, head_cols, rows),
        grid=(batches,),
        in_specs=[one_step(wide, 1), one_step(1, wide), one_step(wide, 3 * width)],
        out_specs=one_step(rows, width),
        out_shape=jax.ShapeDtypeStruct((batches, rows, width), bf16),
    )(id_column, id_row, qkv).reshape(total, width)

    stream = inputs.astype(f32).reshape(total, width)

    def column(values, t, size):
        return values[:, t * size : (t + 1) * size]

    branch = sum(dot(column(mixed, t, head_cols), out_all[t], 1, 1) for t in range(shards))
    middle = stream + branch + out_bias
    hat_two, rate_two = norm_stats(middle)
    normed_two = (hat_two * ln2_gain + ln2_bias).astype(bf16)
    feed_grad = cotangent.reshape(total, width)
    feed = 0.0
    normed_two_grad = 0.0
    up_grads, down_grads, up_sums = [], [], []
    for t in range(shards):
        hidden = dot(normed_two, up_all[t], 1, 0) + up_bias_all[t]
        cdf = (1 + lax.erf(hidden * 0.5**0.5)) * 0.5
        active = (hidden * cdf).astype(bf16)
        feed = feed + dot(active, down_all[t], 1, 1)
        down_grads.append(dot(feed_grad, active, 0, 0).astype(bf16))
        slope = cdf + hidden * jnp.exp(-0.5 * hidden * hidden) * 0.3989422804014327
        hidden_grad = (dot(feed_grad, down_all[t], 1, 0) * slope).astype(bf16)
        up_sums.append(jnp.sum(hidden_grad.astype(f32), 0))
        up_grads.append(dot(normed_two, hidden_grad, 0, 0).astype(bf16))
        normed_two_grad = normed_two_grad + dot(hidden_grad, up_all[t], 1, 1)
    outputs = middle + feed + down_bias

    middle_grad = feed_grad.astype(f32) + norm_back(normed_two_grad, hat_two, rate_two, ln2_gain)
    branch_grad = middle_grad.astype(bf16)
    branch_wide = with_halo(branch_grad.reshape(batches, rows, width), to_left, to_right)
    branch_wide = branch_wide.reshape(batches * wide, width)
    mixed_grad = jnp.concatenate(
        [dot(branch_wide, out_all[t], 1, 0).astype(bf16) for t in range(shards)], 1
    ).reshape(batches, wide, width)
    out_grads = [
        dot(branch_grad, column(mixed, t, head_cols), 0, 0).astype(bf16) for t in range(shards)
    ]
    qkv_grad = pl.pallas_call(
        functools.partial(attend_back_kernel, heads, head_cols, rows),
        grid=(batches,),
        in_specs=[
            one_step(wide, 1),
            one_step(1, wide),
            one_step(wide, 3 * width),
            one_step(wide, width),
        ],
        out_specs=one_step(rows, 3 * width),
        out_shape=jax.ShapeDtypeStruct((batches, rows, 3 * width), bf16),
    )(id_column, id_row, qkv, mixed_grad).reshape(total, 3 * width)
    qkv_grads = [
        dot(normed, column(qkv_grad, t, 3 * head_cols), 0, 0).astype(bf16) for t in range(shards)
    ]
    normed_grad = sum(
        dot(column(qkv_grad, t, 3 * head_cols), qkv_all[t], 1, 1) for t in range(shards)
    )
    hat = hat_wide[:, HALO : HALO + rows].reshape(total, width)
    rate = rate_wide[:, HALO : HALO + rows].reshape(total, 1)
    input_grad = middle_grad + norm_back(normed_grad, hat, rate, ln1_gain)

    def scatter(blocks):
        parts = jnp.stack([block.reshape(replicas, depth, -1) for block in blocks], 1)
        parts = lax.psum_scatter(parts, "dp", scatter_dimension=0, tiled=True)[0]
        return lax.psum_scatter(parts, "tensor", scatter_dimension=0, tiled=True)[0].astype(f32)

    down_share = scatter(down_grads)
    up_share = scatter(up_grads)
    out_share = scatter(out_grads)
    qkv_share = scatter(qkv_grads)
    qkv_sum = jnp.sum(qkv_grad.astype(f32), 0).reshape(shards, 3, head_cols)
    sums = lax.psum(
        jnp.concatenate(
            [
                qkv_sum[:, 0].reshape(-1),
                qkv_sum[:, 2].reshape(-1),
                *up_sums,
                jnp.sum(branch_grad.astype(f32), 0),
                jnp.sum(feed_grad.astype(f32), 0),
                jnp.sum(normed_grad * hat, 0),
                jnp.sum(normed_grad, 0),
                jnp.sum(normed_two_grad * hat_two, 0),
                jnp.sum(normed_two_grad, 0),
            ]
        ),
        ("dp", "tensor"),
    )
    qv_sum = sums[: 2 * width].reshape(2, width)
    up_sum = sums[2 * width : 2 * width + shards * hidden_cols]
    rest = sums[2 * width + shards * hidden_cols :].reshape(6, width)
    return (
        outputs.reshape(batches, rows, width),
        input_grad.reshape(batches, rows, width),
        rest[2],
        rest[3],
        qkv_share.reshape(depth, 3, head_cols).transpose(1, 0, 2),
        qv_sum,
        out_share.T,
        rest[0],
        rest[4],
        rest[5],
        up_share,
        up_sum,
        down_share.T,
        rest[1],
    )


def solution(mesh):
    in_specs = (
        P(None, ("dp", "tensor"), None),
        P(None, ("dp", "tensor"), None),
        P(None, "dp", None),
        P(),
        P(),
        P(None, "dp", "tensor"),
        P(None, "tensor"),
        P("tensor", "dp"),
        P(),
        P(),
        P(),
        P("dp", "tensor"),
        P("tensor"),
        P("tensor", "dp"),
        P(),
    )
    out_specs = (
        P(None, ("dp", "tensor"), None),
        P(None, ("dp", "tensor"), None),
        P(),
        P(),
        P(None, "dp", "tensor"),
        P(),
        P("tensor", "dp"),
        P(),
        P(),
        P(),
        P("dp", "tensor"),
        P(),
        P("tensor", "dp"),
        P(),
    )
    return jax.shard_map(body, mesh=mesh, in_specs=in_specs, out_specs=out_specs, check_vma=False)
```
